32 devices in a mesh: part: 2 (over x), fsdp: 16 (over z, y, core).
Axes of the slice: x: 2, y: 2, z: 4, core: 2. Of those that a mesh axis runs over, the one named last changes fastest.
Arguments:
- acts_in: bfloat16 [2, 16384, 1024], P(None, ('part', 'fsdp')), parts along dimension 1
- cot_out: bfloat16 [2, 16384, 1024], P(None, ('part', 'fsdp')), parts along dimension 1
- lengths: int32 [2, 32], P(None, ('part', 'fsdp')), parts along dimension 1
- w_up: bfloat16 [2, 1024, 4096], replicated
- w_down: bfloat16 [2, 4096, 1024], replicated
Outputs:
- output 1: float32 [4, 1024, 4096], P('part', 'fsdp'), parts along dimension 0
- output 2: float32 [4, 4096, 1024], P('part', 'fsdp'), parts along dimension 0
There are 2 independent parts. The reference program is written for one: setup_inputs(seed, part) draws one part's arguments, and reference() takes and returns one part's arrays. A program takes and returns all parts, laid end to end along the dimension named above; an argument that names none is the same for every part.
All inputs are finite; a program needn't handle non-finite values.
Results may differ from the reference program's by a relative error of at most 0.0097686.
Values are sent between devices in bfloat16 or wider.
A program may use at most 1 GiB of HBM per device.

```python
import jax
import jax.numpy as jnp
from jax import lax

MICRO = 2
TOK = 512
LAYERS = 2
D = 1024
FF = 4096
GROUP = 16

TOKENS = GROUP * TOK
LMIN = TOK // 4


def gelu_fwd(h_wide):
    return jax.nn.gelu(h_wide, approximate=True)


def gelu_back(h_wide, da_val):
    return jax.vjp(gelu_fwd, h_wide)[1](da_val)[0]


def draw_lengths(key_len):
    keys_len = jax.random.split(key_len, 2)
    base_len = jax.random.randint(keys_len[0], (MICRO, GROUP), LMIN, TOK + 1, jnp.int32)
    full_idx = jax.random.randint(keys_len[1], (MICRO, 1), 0, GROUP, jnp.int32)
    short_idx = (full_idx + 1) % GROUP
    col_ids = jnp.arange(GROUP, dtype=jnp.int32)[None, :]
    len_table = jnp.where(col_ids == full_idx, TOK, jnp.where(col_ids == short_idx, LMIN, base_len))
    return len_table.astype(jnp.int32)


def setup_inputs(seed: int = 0, part: int = 0) -> dict:
    key_part = jax.random.fold_in(jax.random.key(seed), part)
    keys_part = jax.random.split(key_part, 3)
    keys_shared = jax.random.split(jax.random.key(seed + 1), 2)
    acts_in = jax.random.normal(keys_part[0], (MICRO, TOKENS, D), jnp.float32)
    cot_out = jax.random.normal(keys_part[1], (MICRO, TOKENS, D), jnp.float32) * (MICRO * TOKENS) ** -0.5
    lengths = draw_lengths(keys_part[2])
    w_up = jax.random.normal(keys_shared[0], (LAYERS, D, FF), jnp.float32) * D ** -0.5
    w_down = jax.random.normal(keys_shared[1], (LAYERS, FF, D), jnp.float32) * FF ** -0.5
    return {
        "acts_in": acts_in.astype(jnp.bfloat16),
        "cot_out": cot_out.astype(jnp.bfloat16),
        "lengths": lengths,
        "w_up": w_up.astype(jnp.bfloat16),
        "w_down": w_down.astype(jnp.bfloat16),
    }


def micro_grads(acts_mb, cot_mb, w_up, w_down):
    def fwd_body(x_cur, weights):
        w_in, w_out = weights
        h_val = jnp.dot(x_cur, w_in, preferred_element_type=jnp.float32).astype(jnp.bfloat16)
        a_val = gelu_fwd(h_val.astype(jnp.float32)).astype(jnp.bfloat16)
        y_val = jnp.dot(a_val, w_out, preferred_element_type=jnp.float32).astype(jnp.bfloat16)
        x_next = (x_cur.astype(jnp.float32) + y_val.astype(jnp.float32)).astype(jnp.bfloat16)
        return x_next, (x_cur, h_val)

    _, (saved_x, saved_h) = lax.scan(fwd_body, acts_mb, (w_up, w_down))

    def bwd_body(dx_cur, layer_items):
        w_in, w_out, x_prev, h_val = layer_items
        h_wide = h_val.astype(jnp.float32)
        a_val = gelu_fwd(h_wide).astype(jnp.bfloat16)
        da_val = jnp.dot(dx_cur, w_out.T, preferred_element_type=jnp.float32)
        dh_val = gelu_back(h_wide, da_val).astype(jnp.bfloat16)
        grad_down = jnp.dot(a_val.T, dx_cur, preferred_element_type=jnp.float32)
        grad_up = jnp.dot(x_prev.T, dh_val, preferred_element_type=jnp.float32)
        dx_back = jnp.dot(dh_val, w_in.T, preferred_element_type=jnp.float32)
        dx_prev = (dx_cur.astype(jnp.float32) + dx_back).astype(jnp.bfloat16)
        return dx_prev, (grad_up, grad_down)

    _, (grads_up, grads_down) = lax.scan(bwd_body, cot_mb, (w_up, w_down, saved_x, saved_h), reverse=True)
    return grads_up, grads_down


def reference(acts_in, cot_out, lengths, w_up, w_down):
    valid_mask = jnp.arange(TOK)[None, None, :] < lengths[:, :, None]
    valid_mask = valid_mask.reshape(MICRO, TOKENS)
    cot_kept = jnp.where(valid_mask[:, :, None], cot_out, jnp.zeros_like(cot_out))

    def body(acc_pair, mb_items):
        acc_up, acc_down = acc_pair
        acts_mb, cot_mb = mb_items
        step_up, step_down = micro_grads(acts_mb, cot_mb, w_up, w_down)
        return (acc_up + step_up, acc_down + step_down), None

    zero_acc = (jnp.zeros((LAYERS, D, FF), jnp.float32), jnp.zeros((LAYERS, FF, D), jnp.float32))
    (grad_up, grad_down), _ = lax.scan(body, zero_acc, (acts_in, cot_kept))
    return grad_up, grad_down
```

```python
import jax
import jax.numpy as jnp
from jax import lax
from jax.sharding import Mesh, PartitionSpec as P


CONTRACT_LAST = (((1,), (1,)), ((), ()))
CONTRACT_FIRST = (((0,), (0,)), ((), ()))


def gelu_fwd(h_wide):
    return jax.nn.gelu(h_wide, approximate=True)


def gelu_back(h_wide, da_val):
    return jax.vjp(gelu_fwd, h_wide)[1](da_val)[0]


def dot_f32(lhs, rhs, dims=(((1,), (0,)), ((), ()))):
    return lax.dot_general(lhs, rhs, dims, preferred_element_type=jnp.float32)


SWAP = [(0, 1), (1, 0)]


def gather_quad(tok):
    other = lax.ppermute(tok, "y", SWAP)
    pair = jnp.concatenate([tok, other], axis=0)
    other = lax.ppermute(pair, "core", SWAP)
    return jnp.concatenate([pair, other], axis=0)


def solution(mesh):
    quad = 4
    n_z = mesh.shape["fsdp"] // quad
    fine = Mesh(mesh.devices.reshape(mesh.shape["part"], n_z, 2, 2), ("part", "z", "y", "core"))
    fsdp = ("z", "y", "core")

    def local_step(acts_in, cot_out, lengths, w_up, w_down):
        micro, tok_rows, width = acts_in.shape
        hidden = w_up.shape[2]
        own = hidden // (n_z * quad)
        q_idx = lax.axis_index("y") * 2 + lax.axis_index("core")
        keep = jnp.arange(tok_rows)[None, :] < lengths
        r_val = jnp.where(keep[:, :, None], cot_out, jnp.zeros_like(cot_out)).reshape(micro * tok_rows, width)
        x_0 = acts_in.reshape(micro * tok_rows, width)

        dx_2_all = gather_quad(r_val)

        h_val = dot_f32(x_0, w_up[0]).astype(jnp.bfloat16)
        a_val = gelu_fwd(h_val.astype(jnp.float32)).astype(jnp.bfloat16)
        y_val = dot_f32(a_val, w_down[0]).astype(jnp.bfloat16)
        x_1 = (x_0.astype(jnp.float32) + y_val.astype(jnp.float32)).astype(jnp.bfloat16)
        x_1_all = gather_quad(x_1)
        x_0_all = gather_quad(x_0)
        h_val = dot_f32(x_1, w_up[1]).astype(jnp.bfloat16)
        da_val = dot_f32(r_val, w_down[1], CONTRACT_LAST)
        dh_val = gelu_back(h_val.astype(jnp.float32), da_val).astype(jnp.bfloat16)
        dx_back = dot_f32(dh_val, w_up[1], CONTRACT_LAST)
        dx_1 = (r_val.astype(jnp.float32) + dx_back).astype(jnp.bfloat16)
        dx_1_all = gather_quad(dx_1)

        def slice_grads(layer, x_all, dx_all):
            cols = [z_idx * quad * own + q_idx * own for z_idx in range(n_z)]
            w_in = [lax.dynamic_slice(w_up, (layer, 0, col), (1, width, own))[0] for col in cols]
            w_in = jnp.concatenate(w_in, axis=1)
            w_out = [lax.dynamic_slice(w_down, (layer, col, 0), (1, own, width))[0] for col in cols]
            w_out = jnp.concatenate(w_out, axis=0)
            h_sl = dot_f32(x_all, w_in).astype(jnp.bfloat16)
            h_wide = h_sl.astype(jnp.float32)
            a_sl = gelu_fwd(h_wide).astype(jnp.bfloat16)
            da_sl = dot_f32(dx_all, w_out, CONTRACT_LAST)
            dh_sl = gelu_back(h_wide, da_sl).astype(jnp.bfloat16)
            part_up = dot_f32(x_all, dh_sl, CONTRACT_FIRST)
            sum_up = lax.psum_scatter(part_up, "z", scatter_dimension=0, tiled=True)
            part_down = dot_f32(a_sl, dx_all, CONTRACT_FIRST)
            sum_down = lax.psum_scatter(part_down, "z", scatter_dimension=0, tiled=True)
            rows = width // (n_z * quad)
            swapped = lax.all_to_all(sum_up.reshape(quad, rows, n_z * own), ("y", "core"), 0, 0)
            full = swapped.reshape(quad, rows, n_z, own).transpose(1, 2, 0, 3).reshape(rows, hidden)
            return full, sum_down

        up_1, down_1 = slice_grads(1, x_1_all, dx_2_all)
        up_0, down_0 = slice_grads(0, x_0_all, dx_1_all)
        return jnp.stack([up_0, up_1]), jnp.stack([down_0, down_1])

    act_spec = P(None, ("part",) + fsdp, None)
    grad_spec = P("part", fsdp, None)
    return jax.shard_map(
        local_step,
        mesh=fine,
        in_specs=(act_spec, act_spec, P(None, ("part",) + fsdp), P(), P()),
        out_specs=(grad_spec, grad_spec),
        check_vma=False,
    )
```
